32 devices in a mesh: agent: 16 (over z, y, x), grid: 2 (over core).
Axes of the slice: x: 2, y: 2, z: 4, core: 2. Of those that a mesh axis runs over, the one named last changes fastest.
Arguments:
- value_prior: float32 [2048, 1024], P(None, 'agent'), may hold values from -6 to 6
- trans_weight: float32 [128, 128], replicated, may hold values from 0.05 to 1
- perceived_law_coefficient: float32 [4], replicated, may hold values from 0.7 to 1
- perceived_law_constant: float32 [4], replicated, may hold values from 0.5 to 4
- interest: float32 [4, 16], replicated, may hold values from 0 to 0.05
- wage_level: float32 [4, 16], replicated, may hold values from 0.5 to 1.5
- efficiency: float32 [32], replicated, may hold values from 0.2 to 3
- holdings: float32 [131072], P('agent'), may hold values from 0 to 40
- shocks: int32 [4, 131072], P(None, 'agent'), may hold values from 0 to 31
- brackets: int32 [4, 131072], P(None, 'agent'), may hold values from 0 to 1022
- aggregate: int32 [4], replicated, may hold values from 0 to 3
Outputs:
- value_new: float32 [2048, 1024], P('agent', 'grid')
- policy: float32 [2048, 1024], P('agent', 'grid')
- holdings_final: float32 [131072], P('agent')
- capital: float32 [4], replicated
The draws below stay inside these ranges and needn't reach their ends.
All inputs are finite; a program needn't handle non-finite values.
Results may differ from the reference program's by a relative error of at most 0.0003.
Values sent between devices are 32-bit elements; how exact they have to be, the bound alone decides.
A program may use at most 64 MiB of HBM per device.

```python
import math
import jax
import jax.numpy as jnp
from jax import lax

A = 1024
E = 32
NK = 16
Z = 4
STATES = 2048
AGENTS = 131072
PERIODS = 4


wealth_upper_limit = 40.0


def bracket_start(key):
    base_key = jax.random.fold_in(key, 7)
    positions = jnp.arange(AGENTS, dtype=jnp.int32)
    stride = max(AGENTS // 1024, 1)
    buckets = (AGENTS + stride - 1) // stride
    bucket = positions // stride
    bracket_top = (A - 1) * 3 // 10 + bucket * ((A - 1) * 7 // 10) // buckets + 1
    return jax.random.randint(base_key, (AGENTS,), 0, bracket_top, dtype=jnp.int32)


def draw_brackets(key, part):
    first_row = bracket_start(key)
    later_rows = jax.random.randint(jax.random.fold_in(key, 9), (PERIODS - 1, AGENTS), 0, A - 1, dtype=jnp.int32)
    return jnp.concatenate([first_row[None, :], later_rows], axis=0)


def draw_holdings(key, part):
    start = bracket_start(key)
    fraction = jax.random.uniform(jax.random.fold_in(key, 11), (AGENTS,), jnp.float32, -0.25, 1.25)
    share_low = start.astype(jnp.float32) / (A - 1)
    share_high = (start + 1).astype(jnp.float32) / (A - 1)
    edge_low = wealth_upper_limit * share_low * share_low
    edge_high = wealth_upper_limit * share_high * share_high
    return jnp.clip(edge_low + fraction * (edge_high - edge_low), 0.0, wealth_upper_limit).astype(jnp.float32)


def place_ends(drawn, stream_key, low, largest):
    longest = drawn.shape.index(max(drawn.shape))
    spots = []
    for shift in (0, 1):
        where = [jax.random.randint(jax.random.fold_in(stream_key, axis), (), 0, length) for axis, length in enumerate(drawn.shape)]
        where[longest] = (where[longest] + shift) % drawn.shape[longest]
        spots.append(tuple(where))
    return drawn.at[spots[0]].set(low).at[spots[1]].set(largest)


def levels(stream_key, shape, cuts, low, largest):
    loudness = 1.0
    for axis_at, parts in cuts:
        steps = jax.random.uniform(jax.random.fold_in(jax.random.fold_in(stream_key, 6), axis_at), (parts,), jnp.float32, low / len(cuts), largest / len(cuts))
        loudness = loudness * jnp.repeat(jnp.exp(steps), shape[axis_at] // parts).reshape((-1,) + (1,) * (len(shape) - 1 - axis_at))
    return loudness


def centred(rng, extent, scale, reach, pieces=(), held_as=jnp.bfloat16):
    gain = levels(rng, extent, pieces, -0.22, 0.18) if pieces else 1.0
    values = jax.random.normal(rng, extent, jnp.float32) * scale * gain
    return jnp.minimum(jnp.maximum(values, -reach), reach).astype(held_as)


def setup_inputs(seed: int = 0) -> dict:
    splits = jax.random.split(jax.random.key(seed), 12)
    value_prior = centred(splits[0], (STATES, A), 1.0, 6.0, ((1, 16),), jnp.float32)
    trans_weight = jnp.clip(jnp.exp(jax.random.uniform(splits[1], (Z * E, Z * E), jnp.float32, math.log(0.05), math.log(1.0))), 0.05, 1.0)
    perceived_law_coefficient = jnp.clip(jnp.exp(jax.random.uniform(splits[2], (Z,), jnp.float32, math.log(0.7), math.log(1.0))), 0.7, 1.0)
    perceived_law_constant = jnp.clip(jax.random.uniform(splits[3], (Z,), jnp.float32, 0.5, 4.0), 0.5, 4.0)
    interest = jnp.clip(jax.random.uniform(splits[4], (Z, NK), jnp.float32, 0.0, 0.05), 0.0, 0.05)
    wage_level = jnp.clip(jax.random.uniform(splits[5], (Z, NK), jnp.float32, 0.5, 1.5), 0.5, 1.5)
    efficiency = jnp.clip(jnp.exp(jax.random.uniform(splits[6], (E,), jnp.float32, math.log(0.2), math.log(3.0))), 0.2, 3.0)
    holdings = draw_holdings(jax.random.fold_in(splits[11], 71), 0)
    shocks = place_ends(jax.random.randint(splits[8], (PERIODS, AGENTS), 0, E), jax.random.fold_in(splits[8], 1), 0, E - 1).astype(jnp.int32)
    brackets = draw_brackets(jax.random.fold_in(splits[11], 71), 0)
    aggregate = place_ends(jax.random.randint(splits[10], (PERIODS,), 0, Z), jax.random.fold_in(splits[10], 1), 0, Z - 1).astype(jnp.int32)
    return {"value_prior": value_prior, "trans_weight": trans_weight, "perceived_law_coefficient": perceived_law_coefficient, "perceived_law_constant": perceived_law_constant, "interest": interest, "wage_level": wage_level, "efficiency": efficiency, "holdings": holdings, "shocks": shocks, "brackets": brackets, "aggregate": aggregate}


wealth_upper_limit = 40.0
beta_disc = 0.96
tau_soft = 0.02
floor_cons = 0.1
highest = lax.Precision.HIGHEST


def make_points():
    fraction = jnp.arange(A, dtype=jnp.float32) / (A - 1)
    return wealth_upper_limit * fraction * fraction


def hat_function_shares(position):
    spacing = wealth_upper_limit / (NK - 1)
    savings_mesh_points = wealth_upper_limit * jnp.arange(NK, dtype=jnp.float32) / (NK - 1)
    return jnp.maximum(0.0, 1.0 - jnp.abs(position[..., None] - savings_mesh_points) / spacing)


def bellman(points, wealth, expected):
    consume = wealth[:, None] - points[None, :]
    clipped = jnp.maximum(consume, floor_cons)
    utility = jnp.log(clipped) + (consume - clipped) / floor_cons
    scores = (utility + beta_disc * expected[None, :]) / tau_soft
    highest_score = jnp.max(scores, axis=1, keepdims=True)
    weight = jnp.exp(scores - highest_score)
    totals = jnp.sum(weight, axis=1)
    values_now = tau_soft * (highest_score[:, 0] + jnp.log(totals))
    chosen = jnp.sum(weight * points[None, :], axis=1) / totals
    return values_now, chosen


def advance(lookup, points, current, shock_row, bracket_row):
    flattened = lookup.reshape(-1)
    flat_index = shock_row * lookup.shape[1] + bracket_row
    value_low = jnp.take(flattened, flat_index)
    value_high = jnp.take(flattened, flat_index + 1)
    edge_low = jnp.take(points, bracket_row)
    edge_high = jnp.take(points, bracket_row + 1)
    fraction = jnp.clip((current - edge_low) / (edge_high - edge_low), 0.0, 1.0)
    return value_low + fraction * (value_high - value_low)


def reference(value_prior, trans_weight, perceived_law_coefficient, perceived_law_constant, interest, wage_level, efficiency, holdings, shocks, brackets, aggregate):
    points = make_points()
    savings_mesh_points = wealth_upper_limit * jnp.arange(NK, dtype=jnp.float32) / (NK - 1)
    predicted_stock = jnp.clip(perceived_law_coefficient[:, None] * savings_mesh_points[None, :] + perceived_law_constant[:, None], 0.0, wealth_upper_limit)
    offset_coefficients = hat_function_shares(predicted_stock)
    transition = trans_weight / jnp.sum(trans_weight, axis=1, keepdims=True)
    value_cube = value_prior.reshape(Z, NK, E, A)
    mixed = jnp.einsum("ykfa,zjk->zjyfa", value_cube, offset_coefficients, precision=highest)
    expected = jnp.einsum("zjyfa,zeyf->zjea", mixed, transition.reshape(Z, E, Z, E), precision=highest).reshape(STATES, A)
    growth = jnp.broadcast_to((1.0 + interest)[:, :, None], (Z, NK, E)).reshape(STATES)
    income = (wage_level[:, :, None] * efficiency[None, None, :]).reshape(STATES)

    def one_state(packed):
        column, factor, earned = packed
        return bellman(points, points * factor + earned, column)

    values_now, policy = lax.map(one_state, (expected, growth, income))
    policy_cube = policy.reshape(Z, NK, E, A)
    current = holdings
    capital_path = []
    for period in range(PERIODS):
        capital = jnp.sum(current) / AGENTS
        capital_path.append(capital)
        sliced = lax.dynamic_index_in_dim(policy_cube, aggregate[period], 0, keepdims=False)
        lookup = jnp.einsum("k,kea->ea", hat_function_shares(capital), sliced, precision=highest)
        current = advance(lookup, points, current, shocks[period], brackets[period])
    return values_now, policy, current, jnp.stack(capital_path)
```

```python
import functools
import math
import jax
import jax.numpy as jnp
from jax import lax
from jax.experimental import pallas as pl
from jax.experimental.pallas import tpu as pltpu
from jax.sharding import PartitionSpec as P

wealth_upper_limit = 40.0
beta_disc = 0.96
tau_soft = 0.02
floor_cons = 0.1
highest = lax.Precision.HIGHEST
LOG2E = 1.0 / math.log(2.0)
SCALE = LOG2E / tau_soft
SLOPE = SCALE / floor_cons
JB = 32
IB = 8


def make_points(count):
    fraction = jnp.arange(count, dtype=jnp.float32) / (count - 1)
    return wealth_upper_limit * fraction * fraction


def hat_function_shares(position, knots):
    spacing = wealth_upper_limit / (knots - 1)
    mesh_points = wealth_upper_limit * jnp.arange(knots, dtype=jnp.float32) / (knots - 1)
    return jnp.maximum(0.0, 1.0 - jnp.abs(position[..., None] - mesh_points) / spacing)


def bellman_kernel(nlog_ref, nall_ref, score_ref, point_ref, wealth_ref, tail_m, tail_t, tail_q, tail_p,
                   value_ref, policy_ref, scratch):
    width = score_ref.shape[1]
    subs = JB // 8

    def group(g, _):
        row = pl.multiple_of(g * IB, IB)
        nlog = nlog_ref[g]
        nall = nall_ref[g]
        wealth = [jnp.broadcast_to(wealth_ref[pl.ds(row + r, 1), :], (8, width)) for r in range(IB)]

        def scores(block, tops, mixed):
            start = pl.multiple_of(block * JB, JB)
            tops = list(tops)
            for k in range(subs):
                at = pl.ds(start + 8 * k, 8)
                p = point_ref[at, :]
                e = score_ref[at, :]
                for r in range(IB):
                    c = wealth[r] - p
                    if mixed:
                        clipped = jnp.maximum(c, floor_cons)
                        s = jnp.log(clipped) * SCALE + ((c - clipped) * SLOPE + e)
                    else:
                        s = jnp.log(c) * SCALE + e
                    scratch[r, at, :] = s
                    tops[r] = jnp.maximum(tops[r], s)
            return tuple(tops)

        tops = tuple(jnp.full((8, width), -3e30, jnp.float32) for _ in range(IB))
        tops = lax.fori_loop(0, nlog, lambda b, t: scores(b, t, False), tops)
        tops = lax.fori_loop(nlog, nall, lambda b, t: scores(b, t, True), tops)
        edge = tail_p[pl.ds(nall, 1), :]
        ends = tail_m[pl.ds(nall, 1), :]
        rows = wealth_ref[pl.ds(row, IB), :]
        tail = (rows - edge) * SLOPE + (ends + SCALE * (math.log(floor_cons) - 1.0))
        top = jnp.concatenate([jnp.max(t, axis=0, keepdims=True) for t in tops], axis=0)
        top = jnp.maximum(top, tail)
        tops = [jnp.broadcast_to(top[r:r + 1, :], (8, width)) for r in range(IB)]

        def weigh(block, sums):
            start = pl.multiple_of(block * JB, JB)
            totals, moments = list(sums[0]), list(sums[1])
            for k in range(subs):
                at = pl.ds(start + 8 * k, 8)
                p = point_ref[at, :]
                for r in range(IB):
                    weight = jnp.exp2(scratch[r, at, :] - tops[r])
                    totals[r] = totals[r] + weight
                    moments[r] = moments[r] + weight * p
            return tuple(totals), tuple(moments)

        zero = tuple(jnp.zeros((8, width), jnp.float32) for _ in range(IB))
        totals, moments = lax.fori_loop(0, nall, weigh, (zero, zero))
        total = jnp.concatenate([jnp.sum(t, axis=0, keepdims=True) for t in totals], axis=0)
        moment = jnp.concatenate([jnp.sum(t, axis=0, keepdims=True) for t in moments], axis=0)
        share = jnp.exp2(tail - top)
        total = total + share * tail_t[pl.ds(nall, 1), :]
        moment = moment + share * tail_q[pl.ds(nall, 1), :]
        value_ref[pl.ds(row, IB), :] = (top * math.log(2.0) + jnp.log(total)) * tau_soft
        policy_ref[pl.ds(row, IB), :] = moment / total
        return 0

    lax.fori_loop(0, wealth_ref.shape[0] // IB, group, 0)


def bellman(points, own_points, growth, income, expected):
    count, width = expected.shape
    half = own_points.shape[0]
    wealth = own_points[:, None] * growth[None, :] + income[None, :]
    scaled = expected * (beta_disc * SCALE)
    grid_points = jnp.broadcast_to(points[:, None], (count, width))
    blocks = count // JB
    starts = points.reshape(blocks, JB)[:, 0]
    ends = points.reshape(blocks, JB)[:, -1]
    spans = wealth.reshape(half // IB, IB * width)
    nlog = jnp.sum(ends[None, :] <= jnp.min(spans, axis=1)[:, None] - floor_cons, axis=1, dtype=jnp.int32)
    nall = jnp.sum(starts[None, :] < jnp.max(spans, axis=1)[:, None] - floor_cons, axis=1, dtype=jnp.int32)
    local = points.reshape(blocks, JB) - starts[:, None]
    slope = scaled.reshape(blocks, JB, width) - SLOPE * local[:, :, None]
    block_m = jnp.max(slope, axis=1)
    block_w = jnp.exp2(slope - block_m[:, None, :])
    block_t = jnp.sum(block_w, axis=1)
    block_q = jnp.sum(block_w * points.reshape(blocks, JB, 1), axis=1)
    later = jnp.arange(blocks)[None, :] >= jnp.arange(blocks)[:, None]
    drop = jnp.where(later, SLOPE * (starts[None, :] - starts[:, None]), 1e30)
    shifted = block_m[None, :, :] - drop[:, :, None]
    tail_m = jnp.max(shifted, axis=1)
    share = jnp.exp2(shifted - tail_m[:, None, :])
    tail_t = jnp.sum(share * block_t[None], axis=1)
    tail_q = jnp.sum(share * block_q[None], axis=1)
    pad = ((0, 8), (0, 0))
    tail_m = jnp.pad(tail_m, pad, constant_values=-1e30)
    tail_t = jnp.pad(tail_t, pad)
    tail_q = jnp.pad(tail_q, pad)
    tail_p = jnp.pad(jnp.broadcast_to(starts[:, None], (blocks, width)), pad)
    vmem = pl.BlockSpec(memory_space=pltpu.VMEM)
    smem = pl.BlockSpec(memory_space=pltpu.SMEM)
    shape = jax.ShapeDtypeStruct((half, width), jnp.float32)
    return pl.pallas_call(
        bellman_kernel,
        out_shape=(shape, shape),
        in_specs=[smem, smem] + [vmem] * 7,
        out_specs=(vmem, vmem),
        scratch_shapes=[pltpu.VMEM((IB, count, width), jnp.float32)],
        name="bellman",
    )(nlog, nall, scaled, grid_points, wealth, tail_m, tail_t, tail_q, tail_p)


def advance_kernel(table_ref, held_ref, shock_ref, bracket_ref, out_ref, count):
    lanes = 128
    tiles = count // lanes
    groups = held_ref.shape[0] // 8
    low_row, low_lane, high_row, high_lane, shares = [], [], [], [], []
    for v in range(groups):
        at = slice(8 * v, 8 * v + 8)
        b = bracket_ref[at, :]
        e = shock_ref[at, :] * tiles
        low_row.append(e + b // lanes)
        low_lane.append(b % lanes)
        high_row.append(e + (b + 1) // lanes)
        high_lane.append((b + 1) % lanes)
        f0 = b.astype(jnp.float32) / (count - 1)
        f1 = (b + 1).astype(jnp.float32) / (count - 1)
        p0 = wealth_upper_limit * f0 * f0
        p1 = wealth_upper_limit * f1 * f1
        shares.append(jnp.clip((held_ref[at, :] - p0) / (p1 - p0), 0.0, 1.0))

    def step(r8, carry):
        lows, highs = list(carry[0]), list(carry[1])
        for q in range(8):
            r = r8 * 8 + q
            row = jnp.broadcast_to(table_ref[pl.ds(r, 1), :], (8, lanes))
            for v in range(groups):
                lows[v] = jnp.where(low_row[v] == r, jnp.take_along_axis(row, low_lane[v], axis=1), lows[v])
                highs[v] = jnp.where(high_row[v] == r, jnp.take_along_axis(row, high_lane[v], axis=1), highs[v])
        return tuple(lows), tuple(highs)

    zero = tuple(jnp.zeros((8, lanes), jnp.float32) for _ in range(groups))
    lows, highs = lax.fori_loop(0, table_ref.shape[0] // 8, step, (zero, zero))
    for v in range(groups):
        out_ref[8 * v:8 * v + 8, :] = lows[v] + shares[v] * (highs[v] - lows[v])


def advance(lookup, current, shock_row, bracket_row):
    kinds, count = lookup.shape
    table = lookup.reshape(kinds * count // 128, 128)
    vmem = pl.BlockSpec(memory_space=pltpu.VMEM)
    return pl.pallas_call(
        functools.partial(advance_kernel, count=count),
        out_shape=jax.ShapeDtypeStruct(current.shape, jnp.float32),
        in_specs=[vmem] * 4,
        out_specs=vmem,
        name="advance",
    )(table, current, shock_row, bracket_row)


def on_device(value_prior, trans_weight, perceived_law_coefficient, perceived_law_constant, interest,
              wage_level, efficiency, holdings, shocks, brackets, aggregate):
    zones, knots = interest.shape
    kinds = efficiency.shape[0]
    states = value_prior.shape[0]
    agent_count = lax.axis_size("agent")
    columns = value_prior.shape[1]
    count = columns * agent_count
    per_device = states // agent_count
    half = count // lax.axis_size("grid")
    first_state = lax.axis_index("agent") * per_device
    points = make_points(count)
    transition = trans_weight / jnp.sum(trans_weight, axis=1, keepdims=True)
    mesh_points = wealth_upper_limit * jnp.arange(knots, dtype=jnp.float32) / (knots - 1)
    predicted = jnp.clip(
        perceived_law_coefficient[:, None] * mesh_points[None, :] + perceived_law_constant[:, None],
        0.0, wealth_upper_limit)
    move = hat_function_shares(predicted, knots)
    cube = value_prior.T.reshape(columns, zones, knots, kinds)
    blended = jnp.einsum("nykf,zeyf->nzke", cube, transition.reshape(zones, kinds, zones, kinds), precision=highest)
    partial_value = jnp.einsum("zjk,nzke->nzje", move, blended, precision=highest).reshape(columns, states)
    expected = lax.all_to_all(partial_value, "agent", split_axis=1, concat_axis=0, tiled=True)
    growth_all = jnp.broadcast_to((1.0 + interest)[:, :, None], (zones, knots, kinds)).reshape(states)
    income_all = (wage_level[:, :, None] * efficiency[None, None, :]).reshape(states)
    growth = lax.dynamic_slice_in_dim(growth_all, first_state, per_device)
    income = lax.dynamic_slice_in_dim(income_all, first_state, per_device)
    own_points = lax.dynamic_slice_in_dim(points, lax.axis_index("grid") * half, half)
    value_t, policy_t = bellman(points, own_points, growth, income, expected)
    values_now, policy = value_t.T, policy_t.T
    agents_total = holdings.shape[0] * agent_count
    policy_cube = lax.all_gather(policy, "agent", axis=0, tiled=True).reshape(zones, knots, kinds, half)
    current = holdings.reshape(-1, 128)
    shock_rows = shocks.reshape(shocks.shape[0], -1, 128)
    bracket_rows = brackets.reshape(shocks.shape[0], -1, 128)
    capital_path = []
    for period in range(shocks.shape[0]):
        capital = lax.psum(jnp.sum(current), "agent") / agents_total
        capital_path.append(capital)
        knot_weights = hat_function_shares(capital, knots)
        sliced = lax.dynamic_index_in_dim(policy_cube, aggregate[period], 0, keepdims=False)
        own = jnp.sum(knot_weights[:, None, None] * sliced, axis=0)
        lookup = lax.all_gather(own, "grid", axis=1, tiled=True)
        current = advance(lookup, current, shock_rows[period], bracket_rows[period])
    return (values_now, policy, current.reshape(-1), jnp.stack(capital_path))


def solution(mesh):
    return jax.shard_map(
        on_device,
        mesh=mesh,
        in_specs=(P(None, "agent"), P(), P(), P(), P(), P(), P(), P("agent"), P(None, "agent"),
                  P(None, "agent"), P()),
        out_specs=(P("agent", "grid"), P("agent", "grid"), P("agent"), P()),
        check_vma=False,
    )
```
